128 devices in a mesh: depth: 2 (over core), row: 16 (over z, x), col: 4 (over y).
Axes of the slice: x: 4, y: 4, z: 4, core: 2. Of those that a mesh axis runs over, the one named last changes fastest.
Arguments:
- right_side: bfloat16 [4, 16, 8, 128, 512], P(None, 'row', ('depth', 'col')), may hold values from -6 to 6
- inverse_diag: bfloat16 [4, 16, 8, 1, 128, 128], P(None, 'row', ('depth', 'col')), may hold values from -2 to 2.5, as said below
- coupling: bfloat16 [3, 16, 1024, 8, 2048], P(None, 'row', None, ('depth', 'col')), may hold values from -0.0625 to 0.0625
- pattern: int32 [3, 16, 8, 8, 16], P(None, 'row', None, ('depth', 'col')), may hold values 0 or 1
Outputs:
- forward_solution: bfloat16 [4, 16, 8, 128, 512], P(None, 'row', ('depth', 'col'))
- solution: bfloat16 [4, 16, 8, 128, 512], P(None, 'row', ('depth', 'col'))
The draws below stay inside these ranges and needn't reach their ends.
Inputs may be any that keep to these rules, and one draw needn't show every extreme that they name: `inverse_diag`: each block is lower triangular with positive diagonal.
All inputs are finite; a program needn't handle non-finite values. No bound on the sum of `pattern` on one device may be relied on, other than what follows from the above.
Results may differ from the reference program's by a relative error of at most 0.025.
Values may be sent and summed in bfloat16 or wider, within the bound.
A program may use at most 128 MiB of HBM per device.

```python
import math
import jax
import jax.numpy as jnp
from jax import lax

BW = 128
LEV = 4
BK = 1
NRHS = 512
SHARES = 8
SHARE_ROWS = 128
LEVEL_BLOCKS = 128
N_ROW = 16


def draw_inverse_diag(key, part):
    full_shape = (LEV, N_ROW, SHARES, BK, BW, BW)
    key_low, key_diag = jax.random.split(key)
    below_mask = jnp.tril(jnp.ones((BW, BW), jnp.float32), -1)
    identity = jnp.eye(BW, dtype=jnp.float32)
    strict_part = jax.random.normal(key_low, full_shape, jnp.float32) * (0.6 / math.sqrt(BW))
    diagonal_part = jax.random.uniform(key_diag, full_shape[:-1], jnp.float32, 0.6, 1.4)
    strict_part = jnp.clip(strict_part, -1.5, 1.5)
    return (strict_part * below_mask + diagonal_part[..., None] * identity).astype(jnp.bfloat16)


def plant(values, own_key, least, top_value):
    longest = values.shape.index(max(values.shape))
    spots = []
    for shift in (0, 1):
        where = [jax.random.randint(jax.random.fold_in(own_key, axis), (), 0, length) for axis, length in enumerate(values.shape)]
        where[longest] = (where[longest] + shift) % values.shape[longest]
        spots.append(tuple(where))
    return values.at[spots[0]].set(least).at[spots[1]].set(top_value)


def levels(rng, dims, pieces, low, high):
    def one(position, blocks):
        heights = jax.random.uniform(jax.random.fold_in(jax.random.fold_in(rng, 6), position), (blocks,), jnp.float32, low / len(pieces), high / len(pieces))
        return jnp.repeat(jnp.exp(heights), dims[position] // blocks).reshape((-1,) + (1,) * (len(dims) - position - 1))

    factor_of = one(*pieces[0])
    for cut in pieces[1:]:
        factor_of = factor_of * one(*cut)
    return factor_of


def bell_draw(rng, extent, spread, bound, cuts=(), kind=jnp.bfloat16):
    entries = spread * jax.random.normal(rng, extent, jnp.float32)
    if cuts:
        entries = entries * levels(rng, extent, cuts, -0.22, 0.18)
    return jnp.clip(entries, -bound, bound).astype(kind)


def setup_inputs(seed: int = 0) -> dict:
    key_of = jax.random.split(jax.random.key(seed), 5)
    right_side = bell_draw(key_of[0], (LEV, N_ROW, SHARES, SHARE_ROWS, NRHS), 1.0, 6.0, ((1, 16), (2, 8)))
    inverse_diag = draw_inverse_diag(jax.random.fold_in(key_of[4], 71), 0)
    coupling = bell_draw(key_of[2], (LEV - 1, N_ROW, SHARES * SHARE_ROWS, SHARES, N_ROW * SHARE_ROWS), (LEVEL_BLOCKS * BW // 2) ** -0.5, 0.0625, ((1, 16), (3, 8)))
    pattern = plant((jax.random.randint(key_of[3], (LEV - 1, N_ROW, SHARES * BK, SHARES, N_ROW * BK), 0, 2) < 1).astype(jnp.int32), jax.random.fold_in(key_of[3], 1), 0, 1)
    return {"right_side": right_side, "inverse_diag": inverse_diag, "coupling": coupling, "pattern": pattern}


def apply_blocks(inverse_level, vector, transposed):
    blocks_in = vector.reshape(N_ROW, SHARES, BK, BW, NRHS).astype(jnp.float32)
    inverse_f = inverse_level.astype(jnp.float32)
    if transposed:
        result = jnp.einsum("rktji,rktjn->rktin", inverse_f, blocks_in)
    else:
        result = jnp.einsum("rktij,rktjn->rktin", inverse_f, blocks_in)
    return result.astype(jnp.bfloat16).reshape(N_ROW, SHARES, BK * BW, NRHS)


def reference(right_side, inverse_diag, coupling, pattern):
    def masked_rows(pair_at, row_at):
        blocks = coupling[pair_at, row_at].reshape(SHARES * BK, BW, SHARES, N_ROW * BK, BW)
        gate = pattern[pair_at, row_at].astype(jnp.bfloat16)[:, None, :, :, None]
        return (blocks * gate).reshape(SHARES * BK * BW, SHARES * N_ROW * BK * BW)

    def upward(pair_at, vector):
        gathered = jnp.transpose(vector, (1, 0, 2, 3)).reshape(SHARES * N_ROW * BK * BW, NRHS)

        def one_row(row_at):
            return jnp.dot(masked_rows(pair_at, row_at), gathered, preferred_element_type=jnp.float32)

        result = lax.map(one_row, jnp.arange(N_ROW, dtype=jnp.int32))
        return result.reshape(N_ROW, SHARES, BK * BW, NRHS)

    def downward(pair_at, vector):
        def step_row(accum, row_at):
            rows_z = lax.dynamic_index_in_dim(vector, row_at, 0, keepdims=False).reshape(SHARES * BK * BW, NRHS)
            term = lax.dot_general(masked_rows(pair_at, row_at), rows_z, (((0,), (0,)), ((), ())), preferred_element_type=jnp.float32)
            return accum + term, None

        start_sum = jnp.zeros((SHARES * N_ROW * BK * BW, NRHS), jnp.float32)
        accum, unused = lax.scan(step_row, start_sum, jnp.arange(N_ROW, dtype=jnp.int32))
        return jnp.transpose(accum.reshape(SHARES, N_ROW, BK * BW, NRHS), (1, 0, 2, 3))

    forward = []
    for level_at in range(LEV):
        source = right_side[level_at]
        if level_at == 0:
            residual = source
        else:
            residual = (source.astype(jnp.float32) - upward(level_at - 1, forward[-1])).astype(jnp.bfloat16)
        forward.append(apply_blocks(inverse_diag[level_at], residual, False))
    backward = [None] * LEV
    for level_at in reversed(range(LEV)):
        known_part = forward[level_at]
        if level_at == LEV - 1:
            residual = known_part
        else:
            residual = (known_part.astype(jnp.float32) - downward(level_at, backward[level_at + 1])).astype(jnp.bfloat16)
        backward[level_at] = apply_blocks(inverse_diag[level_at], residual, True)
    return jnp.stack(forward), jnp.stack(backward)
```

```python
import functools

import jax
import jax.numpy as jnp
from jax import lax
from jax.experimental import pallas as pl
from jax.experimental.pallas import tpu as pltpu
from jax.sharding import PartitionSpec as P

F32 = jnp.float32
BF16 = jnp.bfloat16
W = 128
H = 64
PANELS = 4


def kernel(
    nz, nx, ny, levels,
    b_ref, d_ref, gate_ref, m_hbm,
    f_ref, z_ref,
    mv, xg, ps, pr, own, owny, ys, yr, yg, rs, rr0, rr1, ls, lr, ownb, ft,
    load_sem, send_sem, recv_sem,
):
    pairs = levels - 1
    items = pairs * PANELS
    dd = lax.axis_index("depth")
    rw = lax.axis_index("row")
    yy = lax.axis_index("col")
    zz = rw // nx
    xx = rw % nx

    def x_peer(step):
        return {"row": zz * nx + (xx + step) % nx}

    def z_peer(step):
        return {"row": ((zz + step) % nz) * nx + xx}

    def y_peer(step):
        return {"col": (yy + step) % ny}

    partner = {"depth": 1 - dd}
    peers = (
        [x_peer(k) for k in range(1, nx)]
        + [z_peer(k) for k in range(1, nz)]
        + [y_peer(k) for k in range(1, ny)]
        + [partner]
    )

    for lv in range(pairs):
        pltpu.make_async_copy(m_hbm.at[lv], mv.at[lv], load_sem.at[lv]).start()

    barrier = pltpu.get_barrier_semaphore()
    for peer in peers:
        pl.semaphore_signal(
            barrier, inc=1, device_id=peer, device_id_type=pl.DeviceIdType.MESH
        )
    pl.semaphore_wait(barrier, len(peers))

    def send(src, dst, stage, item, peer):
        pltpu.make_async_remote_copy(
            src_ref=src,
            dst_ref=dst,
            send_sem=send_sem.at[stage, item],
            recv_sem=recv_sem.at[stage, item],
            device_id=peer,
            device_id_type=pl.DeviceIdType.MESH,
        ).start()

    def total(stage, item):
        return (
            xg.at[item, 0, 0 : nx - 1],
            xg.at[item, 0 : nz - 1],
            pr.at[item],
            yr.at[item],
            yr.at[item],
            pr.at[item],
            xg.at[item, 0 : nz - 1],
            xg.at[item, 0, 0 : nx - 1],
        )[stage]

    def arrived(stage, item):
        ref = total(stage, item)
        pltpu.make_async_copy(ref, ref, recv_sem.at[stage, item]).wait()

    def sent(stage, item):
        ref = total(stage, item)
        pltpu.make_async_copy(ref, ref, send_sem.at[stage, item]).wait()

    def columns(panel):
        return pl.ds(pl.multiple_of(panel * W, W), W)

    def f1(item):
        lv, pn = item // PANELS, item % PANELS
        prev = item - PANELS

        def finish(residual):
            value = jnp.dot(d_ref[lv], residual, preferred_element_type=F32).astype(BF16)
            f_ref[lv, :, columns(pn)] = value

            @pl.when(lv < pairs)
            def _():
                xg[item, zz, xx] = value
                for k in range(1, nx):
                    here = xg.at[item, zz, xx, 0:H]
                    send(here, here, 0, item, x_peer(k))
                for k in range(1, nz):
                    here = xg.at[item, zz, xx, H:W]
                    send(here, here, 0, item, z_peer(k))

            ft[item] = value.astype(F32).T.astype(BF16)

        @pl.when(lv == 0)
        def _():
            finish(b_ref[0, :, columns(pn)])

        @pl.when(lv > 0)
        def _():
            arrived(3, prev)
            acc = owny[pn]
            for k in range(ny - 1):
                acc = acc + yr[prev, k].astype(F32)
            finish((b_ref[lv, :, columns(pn)].astype(F32) - acc).astype(BF16))

    def f2(item):
        arrived(0, item)
        for k in range(1, nz):
            here = xg.at[item, zz, :, 0:H]
            send(here, here, 1, item, z_peer(k))
        for k in range(1, nx):
            here = xg.at[item, :, xx, H:W]
            send(here, here, 1, item, x_peer(k))

    def f3(item):
        lv, pn = item // PANELS, item % PANELS
        arrived(1, item)
        far = pl.ds(pl.multiple_of((1 - dd) * (ny * W), ny * W), ny * W)
        near = pl.ds(pl.multiple_of(dd * (ny * W), ny * W), ny * W)
        gathered = xg[item].reshape(nz * nx * W, W)
        part = jnp.dot(mv[lv, far, :], gathered, preferred_element_type=F32)
        ps[item] = part.astype(BF16).reshape(ny, W, W)
        send(ps.at[item], pr.at[item], 2, item, partner)
        part = jnp.dot(mv[lv, near, :], gathered, preferred_element_type=F32)
        own[pn] = part.reshape(ny, W, W)

    def f4(item):
        pn = item % PANELS
        arrived(2, item)
        for k in range(1, ny):
            at = (yy + k) % ny
            ys[item, k - 1] = (own[pn, at] + pr[item, at].astype(F32)).astype(BF16)
            send(ys.at[item, k - 1], yr.at[item, k - 1], 3, item, y_peer(k))
        owny[pn] = own[pn, yy] + pr[item, yy].astype(F32)

    def b1(item):
        step, pn = item // PANELS, item % PANELS
        lv = levels - 1 - step
        prev = item - PANELS

        def finish(residual):
            value = jnp.dot(residual, d_ref[lv], preferred_element_type=F32).astype(BF16)

            @pl.when(step < pairs)
            def _():
                mine = dd * ny + yy
                yg[item, mine] = value
                for k in range(1, ny):
                    here = yg.at[item, mine]
                    send(here, here, 4, item, y_peer(k))

            z_ref[lv, :, columns(pn)] = value.astype(F32).T.astype(BF16)

        @pl.when(step == 0)
        def _():
            finish(ft[lv * PANELS + pn])

        @pl.when(step > 0)
        def _():
            arrived(7, prev)
            acc0 = ownb[pn, 0:H]
            for k in range(nx - 1):
                acc0 = acc0 + lr[prev, 0, k].astype(F32)
            acc1 = ownb[pn, H:W]
            for k in range(nz - 1):
                acc1 = acc1 + lr[prev, 1, k].astype(F32)
            acc = jnp.concatenate([acc0, acc1], axis=0)
            finish((ft[lv * PANELS + pn].astype(F32) - acc).astype(BF16))

    def b2(item):
        arrived(4, item)
        here = yg.at[item, pl.ds(dd * ny, ny)]
        send(here, here, 5, item, partner)

    def b3(item):
        lv = pairs - 1 - item // PANELS
        arrived(5, item)
        solved = jnp.concatenate([yg[item, k] for k in range(2 * ny)], axis=1)
        for k in range(1, nz + 1):
            at = (zz + k) % nz
            span = pl.ds(pl.multiple_of(at * (nx * W), nx * W), nx * W)
            part = jnp.dot(solved, mv[lv, :, span], preferred_element_type=F32).astype(BF16)
            for j in range(nx):
                rs[item, at, j] = part[:, j * W : (j + 1) * W]
            if k < nz:
                send(rs.at[item, at, :, 0:H], rr0.at[item, k - 1], 6, item, z_peer(k))
        for k in range(1, nx):
            at = (xx + k) % nx
            send(rs.at[item, :, at, H:W], rr1.at[item, k - 1], 6, item, x_peer(k))

    def b4(item):
        pn = item % PANELS
        arrived(6, item)
        for k in range(nx):
            at = (xx + k) % nx
            acc = rs[item, zz, at, 0:H].astype(F32)
            for j in range(nz - 1):
                acc = acc + rr0[item, j, at].astype(F32)
            if k == 0:
                ownb[pn, 0:H] = acc
            else:
                ls[item, 0, k - 1] = acc.astype(BF16)
                send(ls.at[item, 0, k - 1], lr.at[item, 0, k - 1], 7, item, x_peer(k))
        for k in range(nz):
            at = (zz + k) % nz
            acc = rs[item, at, xx, H:W].astype(F32)
            for j in range(nx - 1):
                acc = acc + rr1[item, j, at].astype(F32)
            if k == 0:
                ownb[pn, H:W] = acc
            else:
                ls[item, 1, k - 1] = acc.astype(BF16)
                send(ls.at[item, 1, k - 1], lr.at[item, 1, k - 1], 7, item, z_peer(k))

    def mask(lv):
        pltpu.make_async_copy(m_hbm.at[lv], mv.at[lv], load_sem.at[lv]).wait()

        def rows(t, carry):
            span = pl.ds(pl.multiple_of(t * W, W), W)
            gate = gate_ref[lv * (2 * ny) + t].astype(BF16)
            mv[lv, span, :] = mv[lv, span, :] * gate
            return carry

        lax.fori_loop(0, 2 * ny, rows, 0)

    def stage(fn, index, count):
        @pl.when((index >= 0) & (index < count))
        def _():
            fn(index)

    def slot(s, carry):
        j = s - items
        stage(f1, s, items + PANELS)
        stage(f4, s - 3, items)
        stage(f2, s - 1, items)
        stage(f3, s - 2, items)

        @pl.when((s % PANELS == 1) & (s < items))
        def _():
            mask(s // PANELS)

        stage(b2, j - 1, items)
        stage(b1, j, items + PANELS)
        stage(b4, j - 3, items)
        stage(b3, j - 1, items)
        return carry

    lax.fori_loop(0, 2 * items + PANELS, slot, 0)

    def drain(item, carry):
        for st in range(8):
            sent(st, item)
        return carry

    lax.fori_loop(0, items, drain, 0)


def body(nz, nx, ny, right_side, inverse_diag, coupling, pattern):
    levels, rhs = right_side.shape[0], right_side.shape[4]
    pairs = levels - 1
    items = pairs * PANELS
    rows, cols = coupling.shape[2], coupling.shape[4]
    b = right_side.reshape(levels, W, rhs)
    d = inverse_diag.reshape(levels, W, W)
    m = coupling.reshape(pairs, rows, cols)
    gate = jnp.repeat(
        pattern.reshape(pairs * 2 * ny, 1, nz * nx).astype(F32), W, axis=2
    )
    vm = pl.BlockSpec(memory_space=pltpu.VMEM)
    f, z = pl.pallas_call(
        functools.partial(kernel, nz, nx, ny, levels),
        out_shape=[jax.ShapeDtypeStruct((levels, W, rhs), BF16)] * 2,
        in_specs=[vm, vm, vm, pl.BlockSpec(memory_space=pl.ANY)],
        out_specs=[vm, vm],
        scratch_shapes=[
            pltpu.VMEM((pairs, rows, cols), BF16),
            pltpu.VMEM((items, nz, nx, W, W), BF16),
            pltpu.VMEM((items, ny, W, W), BF16),
            pltpu.VMEM((items, ny, W, W), BF16),
            pltpu.VMEM((PANELS, ny, W, W), F32),
            pltpu.VMEM((PANELS, W, W), F32),
            pltpu.VMEM((items, ny - 1, W, W), BF16),
            pltpu.VMEM((items, ny - 1, W, W), BF16),
            pltpu.VMEM((items, 2 * ny, W, W), BF16),
            pltpu.VMEM((items, nz, nx, W, W), BF16),
            pltpu.VMEM((items, nz - 1, nx, H, W), BF16),
            pltpu.VMEM((items, nx - 1, nz, H, W), BF16),
            pltpu.VMEM((items, 2, nx - 1, H, W), BF16),
            pltpu.VMEM((items, 2, nx - 1, H, W), BF16),
            pltpu.VMEM((PANELS, W, W), F32),
            pltpu.VMEM((items + PANELS, W, W), BF16),
            pltpu.SemaphoreType.DMA((pairs,)),
            pltpu.SemaphoreType.DMA((8, items)),
            pltpu.SemaphoreType.DMA((8, items)),
        ],
        compiler_params=pltpu.CompilerParams(
            collective_id=0, has_side_effects=True, vmem_limit_bytes=60 * 1024 * 1024
        ),
    )(b, d, gate, m)
    shape = right_side.shape
    return f.reshape(shape), z.reshape(shape)


def solution(mesh):
    placed = (
        P(None, "row", ("depth", "col"), None, None),
        P(None, "row", ("depth", "col"), None, None, None),
        P(None, "row", None, ("depth", "col"), None),
        P(None, "row", None, ("depth", "col"), None),
    )
    side = round(mesh.shape["row"] ** 0.5)
    return jax.shard_map(
        functools.partial(body, side, side, mesh.shape["col"]),
        mesh=mesh,
        in_specs=placed,
        out_specs=(placed[0], placed[0]),
        check_vma=False,
    )
```

```python
import functools

import jax
import jax.numpy as jnp
from jax import lax
from jax.experimental import pallas as pl
from jax.experimental.pallas import tpu as pltpu
from jax.sharding import PartitionSpec as P

F32 = jnp.float32
BF16 = jnp.bfloat16
W = 128
H = 64
PANELS = 4


def far_first(n):
    return sorted(range(1, n), key=lambda k: -min(k, n - k))


def kernel(
    nz, nx, ny, levels,
    b_hbm, d_hbm, pat_ref, m_hbm,
    f_hbm, z_hbm,
    bv, dv, fo, zo, mv, xg, ownf, ys, yr, yg, rs, rr0, rr1, ls, lr, ownb, ft,
    load_sem, in_sem, out_sem, send_sem, recv_sem,
):
    pairs = levels - 1
    items = pairs * PANELS
    dd = lax.axis_index("depth")
    rw = lax.axis_index("row")
    yy = lax.axis_index("col")
    zz = rw // nx
    xx = rw % nx
    shares = [(flip, k) for k in far_first(ny) for flip in (0, 1)] + [(1, 0)]

    def x_peer(step):
        return {"row": zz * nx + (xx + step) % nx}

    def z_peer(step):
        return {"row": ((zz + step) % nz) * nx + xx}

    def share_peer(flip, step):
        return {"depth": (dd + flip) % 2, "col": (yy + step) % ny}

    peers = (
        [x_peer(k) for k in range(1, nx)]
        + [z_peer(k) for k in range(1, nz)]
        + [share_peer(*share) for share in shares]
    )

    barrier = pltpu.get_barrier_semaphore()
    for peer in peers:
        pl.semaphore_signal(
            barrier, inc=1, device_id=peer, device_id_type=pl.DeviceIdType.MESH
        )

    def load_inputs(lv):
        return (
            pltpu.make_async_copy(b_hbm.at[lv], bv.at[lv], in_sem.at[0, lv]),
            pltpu.make_async_copy(d_hbm.at[lv], dv.at[lv], in_sem.at[1, lv]),
        )

    for lv in range(levels):
        for copy in load_inputs(lv):
            copy.start()
        if lv < pairs:
            pltpu.make_async_copy(m_hbm.at[lv], mv.at[lv], load_sem.at[lv]).start()

    for copy in load_inputs(0):
        copy.wait()
    pl.semaphore_wait(barrier, len(peers))

    def send(src, dst, stage, item, peer):
        pltpu.make_async_remote_copy(
            src_ref=src,
            dst_ref=dst,
            send_sem=send_sem.at[stage, item],
            recv_sem=recv_sem.at[stage, item],
            device_id=peer,
            device_id_type=pl.DeviceIdType.MESH,
        ).start()

    def total(stage, item):
        return (
            xg.at[item, 0, 0 : nx - 1],
            xg.at[item, 0 : nz - 1],
            yr.at[item],
            yr.at[item],
            xg.at[item, 0 : nz - 1],
            xg.at[item, 0, 0 : nx - 1],
        )[stage]

    def arrived(stage, item):
        ref = total(stage, item)
        pltpu.make_async_copy(ref, ref, recv_sem.at[stage, item]).wait()

    def sent(stage, item):
        ref = total(stage, item)
        pltpu.make_async_copy(ref, ref, send_sem.at[stage, item]).wait()

    def columns(panel):
        return pl.ds(pl.multiple_of(panel * W, W), W)

    def output(hbm, buf, which, lv):
        return pltpu.make_async_copy(buf.at[lv], hbm.at[lv], out_sem.at[which, lv])

    def f1(item):
        lv, pn = item // PANELS, item % PANELS
        prev = item - PANELS

        def finish(residual):
            value = jnp.dot(dv[lv], residual, preferred_element_type=F32).astype(BF16)

            @pl.when(lv < pairs)
            def _():
                xg[item, zz, xx] = value
                for k in far_first(nx):
                    here = xg.at[item, zz, xx, 0:H]
                    send(here, here, 0, item, x_peer(k))
                for k in far_first(nz):
                    here = xg.at[item, zz, xx, H:W]
                    send(here, here, 0, item, z_peer(k))

            fo[lv, :, columns(pn)] = value
            ft[item] = value.astype(F32).T.astype(BF16)

            @pl.when(pn == PANELS - 1)
            def _():
                output(f_hbm, fo, 0, lv).start()

        @pl.when(lv == 0)
        def _():
            finish(bv[0, :, columns(pn)])

        @pl.when(lv > 0)
        def _():
            arrived(2, prev)
            acc = ownf[pn]
            for k in range(2 * ny - 1):
                acc = acc + yr[prev, k].astype(F32)
            finish((bv[lv, :, columns(pn)].astype(F32) - acc).astype(BF16))

    def f2(item):
        arrived(0, item)
        for k in far_first(nz):
            here = xg.at[item, zz, :, 0:H]
            send(here, here, 1, item, z_peer(k))
        for k in far_first(nx):
            here = xg.at[item, :, xx, H:W]
            send(here, here, 1, item, x_peer(k))

    def f3(item):
        lv, pn = item // PANELS, item % PANELS
        arrived(1, item)
        gathered = xg[item].reshape(nz * nx * W, W)
        for k in far_first(ny) + [0]:
            at = (yy + k) % ny
            rows = [
                mv[lv, pl.ds(pl.multiple_of((side * ny + at) * W, W), W), :]
                for side in (dd, (dd + 1) % 2)
            ]
            part = jnp.dot(
                jnp.concatenate(rows, axis=0), gathered, preferred_element_type=F32
            )
            for flip in (0, 1):
                block = part[flip * W : (flip + 1) * W]
                if flip == 0 and k == 0:
                    ownf[pn] = block
                else:
                    slot = flip * ny + k - 1
                    ys[item, slot] = block.astype(BF16)
                    send(ys.at[item, slot], yr.at[item, slot], 2, item, share_peer(flip, k))

    def b1(item):
        step, pn = item // PANELS, item % PANELS
        lv = levels - 1 - step
        prev = item - PANELS

        def finish(residual):
            value = jnp.dot(residual, dv[lv], preferred_element_type=F32).astype(BF16)

            @pl.when(step < pairs)
            def _():
                mine = dd * ny + yy
                yg[item, mine] = value
                for share in shares:
                    here = yg.at[item, mine]
                    send(here, here, 3, item, share_peer(*share))

            zo[lv, :, columns(pn)] = value.astype(F32).T.astype(BF16)

            @pl.when(pn == PANELS - 1)
            def _():
                output(z_hbm, zo, 1, lv).start()

        @pl.when(step == 0)
        def _():
            finish(ft[lv * PANELS + pn])

        @pl.when(step > 0)
        def _():
            arrived(5, prev)
            acc0 = ownb[pn, 0:H]
            for k in range(nx - 1):
                acc0 = acc0 + lr[prev, 0, k].astype(F32)
            acc1 = ownb[pn, H:W]
            for k in range(nz - 1):
                acc1 = acc1 + lr[prev, 1, k].astype(F32)
            acc = jnp.concatenate([acc0, acc1], axis=0)
            finish((ft[lv * PANELS + pn].astype(F32) - acc).astype(BF16))

    def b3(item):
        lv = pairs - 1 - item // PANELS
        arrived(3, item)
        solved = jnp.concatenate([yg[item, k] for k in range(2 * ny)], axis=1)
        for at in range(nz):
            span = slice(at * nx * W, (at + 1) * nx * W)
            part = jnp.dot(solved, mv[lv, :, span], preferred_element_type=F32).astype(BF16)
            for j in range(nx):
                rs[item, at, j] = part[:, j * W : (j + 1) * W]
        for k in far_first(nz):
            at = (zz + k) % nz
            send(rs.at[item, at, :, 0:H], rr0.at[item, k - 1], 4, item, z_peer(k))
        for k in far_first(nx):
            at = (xx + k) % nx
            send(rs.at[item, :, at, H:W], rr1.at[item, k - 1], 4, item, x_peer(k))

    def b4(item):
        pn = item % PANELS
        arrived(4, item)
        for k in far_first(nx) + [0]:
            at = (xx + k) % nx
            acc = rs[item, zz, at, 0:H].astype(F32)
            for j in range(nz - 1):
                acc = acc + rr0[item, j, at].astype(F32)
            if k == 0:
                ownb[pn, 0:H] = acc
            else:
                ls[item, 0, k - 1] = acc.astype(BF16)
                send(ls.at[item, 0, k - 1], lr.at[item, 0, k - 1], 5, item, x_peer(k))
        for k in far_first(nz) + [0]:
            at = (zz + k) % nz
            acc = rs[item, at, xx, H:W].astype(F32)
            for j in range(nx - 1):
                acc = acc + rr1[item, j, at].astype(F32)
            if k == 0:
                ownb[pn, H:W] = acc
            else:
                ls[item, 1, k - 1] = acc.astype(BF16)
                send(ls.at[item, 1, k - 1], lr.at[item, 1, k - 1], 5, item, z_peer(k))

    def mask(lv):
        pltpu.make_async_copy(m_hbm.at[lv], mv.at[lv], load_sem.at[lv]).wait()
        cols = nz * nx * W
        spread = (
            lax.broadcasted_iota(jnp.int32, (nz * nx, cols), 1) // W
            == lax.broadcasted_iota(jnp.int32, (nz * nx, cols), 0)
        ).astype(BF16)
        gate = jnp.dot(
            pat_ref[lv].astype(F32).astype(BF16), spread, preferred_element_type=F32
        ).astype(BF16)
        for t in range(2 * ny):
            span = pl.ds(t * W, W)
            mv[lv, span, :] = mv[lv, span, :] * gate[t : t + 1, :]

    def settle(item, stages):
        for st in stages:
            sent(st, item)

    def stage(fn, index, count, *extra):
        @pl.when((index >= 0) & (index < count))
        def _():
            fn(index, *extra)

    def first(item, carry):
        f1(item)
        return carry

    def slot(s, carry):
        j = s - items

        @pl.when(s >= PANELS)
        def _():
            stage(f1, s, items + PANELS)

        stage(b4, j - 3, items)
        stage(b1, j, items + PANELS)
        stage(f2, s - 1, items)

        @pl.when((s % PANELS == 1) & (s < items))
        def _():
            mask(s // PANELS)

        @pl.when(s == 1)
        def _():
            for lv in range(1, levels):
                for copy in load_inputs(lv):
                    copy.wait()

        stage(f3, s - 2, items)
        stage(b3, j - 1, items)
        stage(settle, j - 1, items, (0, 1, 2))
        stage(settle, j - 5, items, (3, 4, 5))
        return carry

    lax.fori_loop(0, PANELS, first, 0)
    lax.fori_loop(1, 2 * items + PANELS, slot, 0)
    for item in range(items - 1, items):
        settle(item, (3, 4, 5))
    for lv in range(levels):
        output(f_hbm, fo, 0, lv).wait()
        output(z_hbm, zo, 1, lv).wait()


def body(nz, nx, ny, right_side, inverse_diag, coupling, pattern):
    levels, rhs = right_side.shape[0], right_side.shape[4]
    pairs = levels - 1
    items = pairs * PANELS
    rows, cols = coupling.shape[2], coupling.shape[4]
    b = right_side.reshape(levels, W, rhs)
    d = inverse_diag.reshape(levels, W, W)
    m = coupling.reshape(pairs, rows, cols)
    pat = pattern.reshape(pairs, 2 * ny, nz * nx)
    hbm = pl.BlockSpec(memory_space=pl.ANY)
    f, z = pl.pallas_call(
        functools.partial(kernel, nz, nx, ny, levels),
        out_shape=[jax.ShapeDtypeStruct((levels, W, rhs), BF16)] * 2,
        in_specs=[hbm, hbm, pl.BlockSpec(memory_space=pltpu.VMEM), hbm],
        out_specs=[hbm, hbm],
        scratch_shapes=[
            pltpu.VMEM((levels, W, rhs), BF16),
            pltpu.VMEM((levels, W, W), BF16),
            pltpu.VMEM((levels, W, rhs), BF16),
            pltpu.VMEM((levels, W, rhs), BF16),
            pltpu.VMEM((pairs, rows, cols), BF16),
            pltpu.VMEM((items, nz, nx, W, W), BF16),
            pltpu.VMEM((PANELS, W, W), F32),
            pltpu.VMEM((items, 2 * ny - 1, W, W), BF16),
            pltpu.VMEM((items, 2 * ny - 1, W, W), BF16),
            pltpu.VMEM((items, 2 * ny, W, W), BF16),
            pltpu.VMEM((items, nz, nx, W, W), BF16),
            pltpu.VMEM((items, nz - 1, nx, H, W), BF16),
            pltpu.VMEM((items, nx - 1, nz, H, W), BF16),
            pltpu.VMEM((items, 2, nx - 1, H, W), BF16),
            pltpu.VMEM((items, 2, nx - 1, H, W), BF16),
            pltpu.VMEM((PANELS, W, W), F32),
            pltpu.VMEM((items + PANELS, W, W), BF16),
            pltpu.SemaphoreType.DMA((pairs,)),
            pltpu.SemaphoreType.DMA((2, levels)),
            pltpu.SemaphoreType.DMA((2, levels)),
            pltpu.SemaphoreType.DMA((6, items)),
            pltpu.SemaphoreType.DMA((6, items)),
        ],
        compiler_params=pltpu.CompilerParams(
            collective_id=0, has_side_effects=True, vmem_limit_bytes=60 * 1024 * 1024
        ),
    )(b, d, pat, m)
    shape = right_side.shape
    return f.reshape(shape), z.reshape(shape)


def solution(mesh):
    placed = (
        P(None, "row", ("depth", "col"), None, None),
        P(None, "row", ("depth", "col"), None, None, None),
        P(None, "row", None, ("depth", "col"), None),
        P(None, "row", None, ("depth", "col"), None),
    )
    side = round(mesh.shape["row"] ** 0.5)
    return jax.shard_map(
        functools.partial(body, side, side, mesh.shape["col"]),
        mesh=mesh,
        in_specs=placed,
        out_specs=(placed[0], placed[0]),
        check_vma=False,
    )
```

```python
import functools

import jax
import jax.numpy as jnp
from jax import lax
from jax.experimental import pallas as pl
from jax.experimental.pallas import tpu as pltpu
from jax.sharding import PartitionSpec as P

F32 = jnp.float32
BF16 = jnp.bfloat16
W = 128
H = 64
PANELS = 4


def far_first(n):
    return sorted(range(1, n), key=lambda k: -min(k, n - k))


def kernel(
    nz, nx, ny, levels,
    b_hbm, d_hbm, pat_hbm, m_hbm,
    fo, zo,
    bv, dv, pat, gate, mv, mt, xg, ownf, yf, ys, yr, yg, rs, rr0, rr1, ls, lr, ownb, ft,
    load_sem, in_sem, pat_sem, send_sem, recv_sem,
):
    pairs = levels - 1
    items = pairs * PANELS
    dd = lax.axis_index("depth")
    rw = lax.axis_index("row")
    yy = lax.axis_index("col")
    zz = rw // nx
    xx = rw % nx
    shares = [(flip, k) for k in far_first(ny) for flip in (0, 1)] + [(1, 0)]

    def x_peer(step):
        return {"row": zz * nx + (xx + step) % nx}

    def z_peer(step):
        return {"row": ((zz + step) % nz) * nx + xx}

    def share_peer(flip, step):
        return {"depth": (dd + flip) % 2, "col": (yy + step) % ny}

    peers = (
        [x_peer(k) for k in range(1, nx)]
        + [z_peer(k) for k in range(1, nz)]
        + [share_peer(*share) for share in shares]
    )

    barrier = pltpu.get_barrier_semaphore()
    for peer in peers:
        pl.semaphore_signal(
            barrier, inc=1, device_id=peer, device_id_type=pl.DeviceIdType.MESH
        )

    def load_coupling(lv):
        return pltpu.make_async_copy(m_hbm.at[lv], mv.at[lv], load_sem.at[lv])

    def load_inputs(lv):
        return (
            pltpu.make_async_copy(b_hbm.at[lv], bv.at[lv], in_sem.at[0, lv]),
            pltpu.make_async_copy(d_hbm.at[lv], dv.at[lv], in_sem.at[1, lv]),
        )

    load_pattern = pltpu.make_async_copy(pat_hbm, pat, pat_sem)
    load_pattern.start()
    for lv in range(levels):
        for copy in load_inputs(lv):
            copy.start()
        if lv < pairs:
            load_coupling(lv).start()

    for copy in load_inputs(0):
        copy.wait()
    pl.semaphore_wait(barrier, len(peers))

    def send(src, dst, stage, item, peer):
        pltpu.make_async_remote_copy(
            src_ref=src,
            dst_ref=dst,
            send_sem=send_sem.at[stage, item],
            recv_sem=recv_sem.at[stage, item],
            device_id=peer,
            device_id_type=pl.DeviceIdType.MESH,
        ).start()

    def total(stage, item):
        return (
            xg.at[item, 0, 0 : nx - 1],
            xg.at[item, 0 : nz - 1],
            yr.at[item],
            yr.at[item],
            xg.at[item, 0 : nz - 1],
            xg.at[item, 0, 0 : nx - 1],
        )[stage]

    def arrived(stage, item):
        ref = total(stage, item)
        pltpu.make_async_copy(ref, ref, recv_sem.at[stage, item]).wait()

    def sent(stage, item):
        ref = total(stage, item)
        pltpu.make_async_copy(ref, ref, send_sem.at[stage, item]).wait()

    def columns(panel):
        return pl.ds(pl.multiple_of(panel * W, W), W)

    def f1(item):
        lv, pn = item // PANELS, item % PANELS
        prev = item - PANELS

        def finish(residual):
            value = lax.dot_general(
                residual, dv[lv], (((1,), (1,)), ((), ())), preferred_element_type=F32
            ).astype(BF16)

            @pl.when(lv < pairs)
            def _():
                xg[item, zz, xx] = value
                for k in far_first(nx):
                    here = xg.at[item, zz, xx, 0:H]
                    send(here, here, 0, item, x_peer(k))
                for k in far_first(nz):
                    here = xg.at[item, zz, xx, H:W]
                    send(here, here, 0, item, z_peer(k))

            ft[item] = value
            fo[lv, :, columns(pn)] = value.astype(F32).T.astype(BF16)

        given = bv[lv, :, columns(pn)].astype(F32).T

        @pl.when(lv == 0)
        def _():
            finish(given.astype(BF16))

        @pl.when(lv > 0)
        def _():
            arrived(2, prev)
            acc = ownf[pn]
            for k in range(2 * ny - 1):
                acc = acc + yr[prev, k].astype(F32)
            finish((given - acc).astype(BF16))

    def f2(item):
        arrived(0, item)
        for k in far_first(nz):
            here = xg.at[item, zz, :, 0:H]
            send(here, here, 1, item, z_peer(k))
        for k in far_first(nx):
            here = xg.at[item, :, xx, H:W]
            send(here, here, 1, item, x_peer(k))

    def f3(item):
        lv, pn = item // PANELS, item % PANELS

        @pl.when(item >= PANELS)
        def _():
            sent(2, item - PANELS)

        arrived(1, item)
        solved = jnp.concatenate(
            [xg[item, i, j] for i in range(nz) for j in range(nx)], axis=1
        )
        for side in (0, 1):
            span = slice(side * ny * W, (side + 1) * ny * W)
            part = jnp.dot(solved, mt[lv, :, span], preferred_element_type=F32)
            for j in range(ny):
                yf[side * ny + j] = part[:, j * W : (j + 1) * W]
            for k in far_first(ny):
                slot = (dd + side) % 2 * ny + k - 1
                ys[pn, slot] = yf[side * ny + (yy + k) % ny].astype(BF16)
                send(
                    ys.at[pn, slot], yr.at[item, slot], 2, item,
                    share_peer((dd + side) % 2, k),
                )
        ys[pn, ny - 1] = yf[(1 - dd) * ny + yy].astype(BF16)
        send(ys.at[pn, ny - 1], yr.at[item, ny - 1], 2, item, share_peer(1, 0))
        ownf[pn] = yf[dd * ny + yy]

    def b1(item):
        step, pn = item // PANELS, item % PANELS
        lv = levels - 1 - step
        prev = item - PANELS

        def finish(residual):
            value = jnp.dot(residual, dv[lv], preferred_element_type=F32).astype(BF16)

            @pl.when(step < pairs)
            def _():
                mine = dd * ny + yy
                yg[item, mine] = value
                here = yg.at[item, mine]
                for k in far_first(ny):
                    for side in (0, 1):
                        send(here, here, 3, item, share_peer((dd + side) % 2, k))
                send(here, here, 3, item, share_peer(1, 0))

            zo[lv, :, columns(pn)] = value.astype(F32).T.astype(BF16)

        @pl.when(step == 0)
        def _():
            finish(ft[lv * PANELS + pn])

        @pl.when(step > 0)
        def _():
            arrived(5, prev)
            acc0 = ownb[pn, 0:H]
            for k in range(nx - 1):
                acc0 = acc0 + lr[prev, 0, k].astype(F32)
            acc1 = ownb[pn, H:W]
            for k in range(nz - 1):
                acc1 = acc1 + lr[prev, 1, k].astype(F32)
            acc = jnp.concatenate([acc0, acc1], axis=0)
            finish((ft[lv * PANELS + pn].astype(F32) - acc).astype(BF16))

    def b3(item):
        lv, pn = pairs - 1 - item // PANELS, item % PANELS

        @pl.when(item >= PANELS)
        def _():
            sent(4, item - PANELS)

        arrived(3, item)
        solved = jnp.concatenate([yg[item, k] for k in range(2 * ny)], axis=1)
        for at in range(nz):
            span = slice(at * nx * W, (at + 1) * nx * W)
            part = jnp.dot(solved, mv[lv, :, span], preferred_element_type=F32).astype(BF16)
            for j in range(nx):
                rs[pn, at, j] = part[:, j * W : (j + 1) * W]
        for k in far_first(nz):
            at = (zz + k) % nz
            send(rs.at[pn, at, :, 0:H], rr0.at[item, k - 1], 4, item, z_peer(k))
        for k in far_first(nx):
            at = (xx + k) % nx
            send(rs.at[pn, :, at, H:W], rr1.at[item, k - 1], 4, item, x_peer(k))

    def b4(item):
        pn = item % PANELS
        arrived(4, item)
        for k in far_first(nx) + [0]:
            at = (xx + k) % nx
            acc = rs[pn, zz, at, 0:H].astype(F32)
            for j in range(nz - 1):
                acc = acc + rr0[item, j, at].astype(F32)
            if k == 0:
                ownb[pn, 0:H] = acc
            else:
                ls[item, 0, k - 1] = acc.astype(BF16)
                send(ls.at[item, 0, k - 1], lr.at[item, 0, k - 1], 5, item, x_peer(k))
        for k in far_first(nz) + [0]:
            at = (zz + k) % nz
            acc = rs[pn, at, xx, H:W].astype(F32)
            for j in range(nx - 1):
                acc = acc + rr1[item, j, at].astype(F32)
            if k == 0:
                ownb[pn, H:W] = acc
            else:
                ls[item, 1, k - 1] = acc.astype(BF16)
                send(ls.at[item, 1, k - 1], lr.at[item, 1, k - 1], 5, item, z_peer(k))

    def spread_pattern():
        cols = nz * nx * W
        spread = (
            lax.broadcasted_iota(jnp.int32, (nz * nx, cols), 1) // W
            == lax.broadcasted_iota(jnp.int32, (nz * nx, cols), 0)
        ).astype(BF16)
        for lv in range(pairs):
            rows = jnp.dot(
                pat[lv].astype(F32).astype(BF16), spread, preferred_element_type=F32
            )
            for t in range(2 * ny):
                gate[lv, t] = rows[t : t + 1, :]

    def mask(lv, quarter):
        for t in range(2 * ny // 4):
            row = quarter * (2 * ny // 4) + t
            span = pl.ds(pl.multiple_of(row * W, W), W)
            gated = mv[lv, span, :] * gate[lv, row].astype(BF16)
            mv[lv, span, :] = gated
            mt[lv, :, span] = gated.T

    def settle(item, stages):
        for st in stages:
            sent(st, item)

    def stage(fn, index, count, *extra):
        @pl.when((index >= 0) & (index < count))
        def _():
            fn(index, *extra)

    def first(item, carry):
        f1(item)
        return carry

    def slot(s, carry):
        j = s - items

        @pl.when(s >= PANELS)
        def _():
            stage(f1, s, items + PANELS)

        stage(b4, j - 3, items)
        stage(b1, j, items + PANELS)
        stage(f2, s - 1, items)

        ahead = s + PANELS - 2

        @pl.when((ahead >= PANELS) & (ahead < items))
        def _():
            @pl.when(ahead % PANELS == 0)
            def _():
                load_coupling(ahead // PANELS).wait()

            mask(ahead // PANELS, ahead % PANELS)

        @pl.when(s == 1)
        def _():
            load_coupling(0).wait()
            for quarter in range(4):
                mask(0, quarter)

        stage(f3, s - 2, items)
        stage(b3, j - 1, items)
        stage(settle, j - 1, items, (0, 1))
        stage(settle, j - 5, items, (3, 5))
        return carry

    lax.fori_loop(0, PANELS, first, 0)
    load_pattern.wait()
    spread_pattern()
    for lv in range(1, levels):
        for copy in load_inputs(lv):
            copy.wait()
    lax.fori_loop(1, 2 * items + PANELS, slot, 0)
    settle(items - 1, (3, 5))
    for item in range(items - PANELS, items):
        settle(item, (2, 4))

def store(f_in, z_in, f_out, z_out, sem):
    copies = (
        pltpu.make_async_copy(f_in, f_out, sem.at[0]),
        pltpu.make_async_copy(z_in, z_out, sem.at[1]),
    )
    for copy in copies:
        copy.start()
    for copy in copies:
        copy.wait()


def body(nz, nx, ny, right_side, inverse_diag, coupling, pattern):
    levels, rhs = right_side.shape[0], right_side.shape[4]
    pairs = levels - 1
    items = pairs * PANELS
    rows, cols = coupling.shape[2], coupling.shape[4]
    b = right_side.reshape(levels, W, rhs)
    d = inverse_diag.reshape(levels, W, W)
    m = coupling.reshape(pairs, rows, cols)
    gate = pattern.reshape(pairs, 2 * ny, nz * nx)
    hbm = pl.BlockSpec(memory_space=pltpu.HBM)
    vm = pl.BlockSpec(memory_space=pltpu.VMEM)
    b, d, gate = (pltpu.with_memory_space_constraint(x, pltpu.HBM) for x in (b, d, gate))
    f, z = pl.pallas_call(
        functools.partial(kernel, nz, nx, ny, levels),
        out_shape=[jax.ShapeDtypeStruct((levels, W, rhs), BF16)] * 2,
        in_specs=[hbm, hbm, hbm, hbm],
        out_specs=[vm, vm],
        scratch_shapes=[
            pltpu.VMEM((levels, W, rhs), BF16),
            pltpu.VMEM((levels, W, W), BF16),
            pltpu.VMEM((pairs, 2 * ny, nz * nx), jnp.int32),
            pltpu.VMEM((pairs, 2 * ny, 1, cols), F32),
            pltpu.VMEM((pairs, rows, cols), BF16),
            pltpu.VMEM((pairs, cols, rows), BF16),
            pltpu.VMEM((items, nz, nx, W, W), BF16),
            pltpu.VMEM((PANELS, W, W), F32),
            pltpu.VMEM((2 * ny, W, W), F32),
            pltpu.VMEM((PANELS, 2 * ny - 1, W, W), BF16),
            pltpu.VMEM((items, 2 * ny - 1, W, W), BF16),
            pltpu.VMEM((items, 2 * ny, W, W), BF16),
            pltpu.VMEM((PANELS, nz, nx, W, W), BF16),
            pltpu.VMEM((items, nz - 1, nx, H, W), BF16),
            pltpu.VMEM((items, nx - 1, nz, H, W), BF16),
            pltpu.VMEM((items, 2, nx - 1, H, W), BF16),
            pltpu.VMEM((items, 2, nx - 1, H, W), BF16),
            pltpu.VMEM((PANELS, W, W), F32),
            pltpu.VMEM((items + PANELS, W, W), BF16),
            pltpu.SemaphoreType.DMA((pairs,)),
            pltpu.SemaphoreType.DMA((2, levels)),
            pltpu.SemaphoreType.DMA,
            pltpu.SemaphoreType.DMA((6, items)),
            pltpu.SemaphoreType.DMA((6, items)),
        ],
        compiler_params=pltpu.CompilerParams(
            collective_id=0, has_side_effects=True, vmem_limit_bytes=50 * 1024 * 1024
        ),
    )(b, d, gate, m)
    shape = right_side.shape
    anywhere = pl.BlockSpec(memory_space=pl.ANY)
    f, z = pl.pallas_call(
        store,
        out_shape=[jax.ShapeDtypeStruct((levels, W, rhs), BF16)] * 2,
        in_specs=[anywhere, anywhere],
        out_specs=[anywhere, anywhere],
        scratch_shapes=[pltpu.SemaphoreType.DMA((2,))],
        compiler_params=pltpu.CompilerParams(vmem_limit_bytes=50 * 1024 * 1024),
    )(f, z)
    return f.reshape(shape), z.reshape(shape)


def solution(mesh):
    placed = (
        P(None, "row", ("depth", "col"), None, None),
        P(None, "row", ("depth", "col"), None, None, None),
        P(None, "row", None, ("depth", "col"), None),
        P(None, "row", None, ("depth", "col"), None),
    )
    side = round(mesh.shape["row"] ** 0.5)
    return jax.shard_map(
        functools.partial(body, side, side, mesh.shape["col"]),
        mesh=mesh,
        in_specs=placed,
        out_specs=(placed[0], placed[0]),
        check_vma=False,
    )
```

```python
import functools

import jax
import jax.numpy as jnp
from jax import lax
from jax.experimental import pallas as pl
from jax.experimental.pallas import tpu as pltpu
from jax.sharding import PartitionSpec as P

F32 = jnp.float32
BF16 = jnp.bfloat16
W = 128
H = 64
PANELS = 4


def far_first(n):
    return sorted(range(1, n), key=lambda k: -min(k, n - k))


def kernel(
    nz, nx, ny, levels,
    b_hbm, d_hbm, pat_hbm, m_hbm,
    fo, zo,
    bv, dv, pat, gate, mv, mt, xg, ownf, yf, ys, yr, yg, rs, rr0, rr1, ls, lr, ownb, ft,
    load_sem, in_sem, pat_sem, send_sem, recv_sem,
):
    pairs = levels - 1
    items = pairs * PANELS
    dd = lax.axis_index("depth")
    rw = lax.axis_index("row")
    yy = lax.axis_index("col")
    zz = rw // nx
    xx = rw % nx
    shares = [(flip, k) for k in far_first(ny) for flip in (0, 1)] + [(1, 0)]

    def x_peer(step):
        return {"row": zz * nx + (xx + step) % nx}

    def z_peer(step):
        return {"row": ((zz + step) % nz) * nx + xx}

    def share_peer(flip, step):
        return {"depth": (dd + flip) % 2, "col": (yy + step) % ny}

    peers = (
        [x_peer(k) for k in range(1, nx)]
        + [z_peer(k) for k in range(1, nz)]
        + [share_peer(*share) for share in shares]
    )

    barrier = pltpu.get_barrier_semaphore()
    for peer in peers:
        pl.semaphore_signal(
            barrier, inc=1, device_id=peer, device_id_type=pl.DeviceIdType.MESH
        )

    def load_coupling(lv):
        return pltpu.make_async_copy(m_hbm.at[lv], mv.at[lv], load_sem.at[lv])

    def load_inputs(lv):
        return (
            pltpu.make_async_copy(b_hbm.at[lv], bv.at[lv], in_sem.at[0, lv]),
            pltpu.make_async_copy(d_hbm.at[lv], dv.at[lv], in_sem.at[1, lv]),
        )

    load_pattern = pltpu.make_async_copy(pat_hbm, pat, pat_sem)
    load_pattern.start()
    for lv in range(levels):
        for copy in load_inputs(lv):
            copy.start()
        if lv < pairs:
            load_coupling(lv).start()

    for copy in load_inputs(0):
        copy.wait()
    pl.semaphore_wait(barrier, len(peers))

    def send(src, dst, stage, item, peer):
        pltpu.make_async_remote_copy(
            src_ref=src,
            dst_ref=dst,
            send_sem=send_sem.at[stage, item],
            recv_sem=recv_sem.at[stage, item],
            device_id=peer,
            device_id_type=pl.DeviceIdType.MESH,
        ).start()

    def total(stage, item):
        return (
            xg.at[item, 0, 0 : nx - 1],
            xg.at[item, 0 : nz - 1],
            yr.at[item],
            yr.at[item],
            xg.at[item, 0 : nz - 1],
            xg.at[item, 0, 0 : nx - 1],
        )[stage]

    def arrived(stage, item):
        ref = total(stage, item)
        pltpu.make_async_copy(ref, ref, recv_sem.at[stage, item]).wait()

    def sent(stage, item):
        ref = total(stage, item)
        pltpu.make_async_copy(ref, ref, send_sem.at[stage, item]).wait()

    def columns(panel):
        return pl.ds(pl.multiple_of(panel * W, W), W)

    def f1(item):
        lv, pn = item // PANELS, item % PANELS
        prev = item - PANELS

        def finish(residual):
            value = lax.dot_general(
                residual, dv[lv], (((1,), (1,)), ((), ())), preferred_element_type=F32
            ).astype(BF16)

            @pl.when(lv < pairs)
            def _():
                xg[item, zz, xx] = value
                for k in far_first(nx):
                    here = xg.at[item, zz, xx, 0:H]
                    send(here, here, 0, item, x_peer(k))
                for k in far_first(nz):
                    here = xg.at[item, zz, xx, H:W]
                    send(here, here, 0, item, z_peer(k))

            ft[item] = value
            fo[lv, :, columns(pn)] = value.astype(F32).T.astype(BF16)

        given = bv[lv, :, columns(pn)].astype(F32).T

        @pl.when(lv == 0)
        def _():
            finish(given.astype(BF16))

        @pl.when(lv > 0)
        def _():
            arrived(2, prev)
            acc = ownf[pn]
            for k in range(2 * ny - 1):
                acc = acc + yr[prev, k].astype(F32)
            finish((given - acc).astype(BF16))

    def f2(item):
        arrived(0, item)
        for k in far_first(nz):
            here = xg.at[item, zz, :, 0:H]
            send(here, here, 1, item, z_peer(k))
        for k in far_first(nx):
            here = xg.at[item, :, xx, H:W]
            send(here, here, 1, item, x_peer(k))

    def f3(item):
        lv, pn = item // PANELS, item % PANELS

        @pl.when(item >= PANELS)
        def _():
            sent(2, item - PANELS)

        arrived(1, item)
        solved = jnp.concatenate(
            [xg[item, i, j] for i in range(nz) for j in range(nx)], axis=1
        )
        for side in (0, 1):
            span = slice(side * ny * W, (side + 1) * ny * W)
            part = jnp.dot(solved, mt[lv, :, span], preferred_element_type=F32)
            for j in range(ny):
                yf[side * ny + j] = part[:, j * W : (j + 1) * W]
            for k in far_first(ny):
                slot = (dd + side) % 2 * ny + k - 1
                ys[pn, slot] = yf[side * ny + (yy + k) % ny].astype(BF16)
                send(
                    ys.at[pn, slot], yr.at[item, slot], 2, item,
                    share_peer((dd + side) % 2, k),
                )
        ys[pn, ny - 1] = yf[(1 - dd) * ny + yy].astype(BF16)
        send(ys.at[pn, ny - 1], yr.at[item, ny - 1], 2, item, share_peer(1, 0))
        ownf[pn] = yf[dd * ny + yy]

    def b1(item):
        step, pn = item // PANELS, item % PANELS
        lv = levels - 1 - step
        prev = item - PANELS

        def finish(residual):
            value = jnp.dot(residual, dv[lv], preferred_element_type=F32).astype(BF16)

            @pl.when(step < pairs)
            def _():
                mine = dd * ny + yy
                yg[item, mine] = value
                here = yg.at[item, mine]
                for k in far_first(ny):
                    for side in (0, 1):
                        send(here, here, 3, item, share_peer((dd + side) % 2, k))
                send(here, here, 3, item, share_peer(1, 0))

            zo[lv, :, columns(pn)] = value.astype(F32).T.astype(BF16)

        @pl.when(step == 0)
        def _():
            finish(ft[lv * PANELS + pn])

        @pl.when(step > 0)
        def _():
            arrived(5, prev)
            acc0 = ownb[pn, 0:H]
            for k in range(nx - 1):
                acc0 = acc0 + lr[prev, 0, k].astype(F32)
            acc1 = ownb[pn, H:W]
            for k in range(nz - 1):
                acc1 = acc1 + lr[prev, 1, k].astype(F32)
            acc = jnp.concatenate([acc0, acc1], axis=0)
            finish((ft[lv * PANELS + pn].astype(F32) - acc).astype(BF16))

    def b3(item):
        lv, pn = pairs - 1 - item // PANELS, item % PANELS

        @pl.when(item >= PANELS)
        def _():
            sent(4, item - PANELS)

        arrived(3, item)
        solved = jnp.concatenate([yg[item, k] for k in range(2 * ny)], axis=1)
        for at in range(nz):
            span = slice(at * nx * W, (at + 1) * nx * W)
            part = jnp.dot(solved, mv[lv, :, span], preferred_element_type=F32).astype(BF16)
            for j in range(nx):
                rs[pn, at, j] = part[:, j * W : (j + 1) * W]
        for k in far_first(nz):
            at = (zz + k) % nz
            send(rs.at[pn, at, :, 0:H], rr0.at[item, k - 1], 4, item, z_peer(k))
        for k in far_first(nx):
            at = (xx + k) % nx
            send(rs.at[pn, :, at, H:W], rr1.at[item, k - 1], 4, item, x_peer(k))

    def b4(item):
        pn = item % PANELS
        arrived(4, item)
        for k in far_first(nx) + [0]:
            at = (xx + k) % nx
            acc = rs[pn, zz, at, 0:H].astype(F32)
            for j in range(nz - 1):
                acc = acc + rr0[item, j, at].astype(F32)
            if k == 0:
                ownb[pn, 0:H] = acc
            else:
                ls[item, 0, k - 1] = acc.astype(BF16)
                send(ls.at[item, 0, k - 1], lr.at[item, 0, k - 1], 5, item, x_peer(k))
        for k in far_first(nz) + [0]:
            at = (zz + k) % nz
            acc = rs[pn, at, xx, H:W].astype(F32)
            for j in range(nx - 1):
                acc = acc + rr1[item, j, at].astype(F32)
            if k == 0:
                ownb[pn, H:W] = acc
            else:
                ls[item, 1, k - 1] = acc.astype(BF16)
                send(ls.at[item, 1, k - 1], lr.at[item, 1, k - 1], 5, item, z_peer(k))

    def spread_pattern():
        cols = nz * nx * W
        spread = (
            lax.broadcasted_iota(jnp.int32, (nz * nx, cols), 1) // W
            == lax.broadcasted_iota(jnp.int32, (nz * nx, cols), 0)
        ).astype(BF16)
        for lv in range(pairs):
            rows = jnp.dot(
                pat[lv].astype(F32).astype(BF16), spread, preferred_element_type=F32
            )
            for t in range(2 * ny):
                gate[lv, t] = rows[t : t + 1, :]

    def mask(lv, quarter):
        for t in range(2 * ny // 4):
            row = quarter * (2 * ny // 4) + t
            span = pl.ds(pl.multiple_of(row * W, W), W)
            gated = mv[lv, span, :] * gate[lv, row].astype(BF16)
            mv[lv, span, :] = gated
            mt[lv, :, span] = gated.T

    def settle(item, stages):
        for st in stages:
            sent(st, item)

    def stage(fn, index, count, *extra):
        @pl.when((index >= 0) & (index < count))
        def _():
            fn(index, *extra)

    def first(item, carry):
        f1(item)
        return carry

    def second(item, carry):
        f2(item)
        return carry

    def slot(s, carry):
        j = s - items

        stage(b4, j - 3, items)
        @pl.when(s >= PANELS)
        def _():
            stage(f1, s, items + PANELS)

        stage(b1, j, items + PANELS)
        @pl.when(s > PANELS)
        def _():
            stage(f2, s - 1, items)


        ahead = s + PANELS - 2

        @pl.when((ahead >= PANELS) & (ahead < items))
        def _():
            @pl.when(ahead % PANELS == 0)
            def _():
                load_coupling(ahead // PANELS).wait()

            mask(ahead // PANELS, ahead % PANELS)

        @pl.when(s == 1)
        def _():
            lax.fori_loop(0, PANELS, second, 0)
            load_coupling(0).wait()
            for quarter in range(4):
                mask(0, quarter)

        stage(f3, s - 2, items)
        stage(b3, j - 1, items)
        stage(settle, j - 1, items, (0, 1))
        stage(settle, j - 5, items, (3, 5))
        return carry

    lax.fori_loop(0, PANELS, first, 0)
    load_pattern.wait()
    spread_pattern()
    for lv in range(1, levels):
        for copy in load_inputs(lv):
            copy.wait()
    lax.fori_loop(1, 2 * items + PANELS, slot, 0)
    settle(items - 1, (3, 5))
    for item in range(items - PANELS, items):
        settle(item, (2, 4))

def store(f_in, z_in, f_out, z_out, sem):
    copies = (
        pltpu.make_async_copy(f_in, f_out, sem.at[0]),
        pltpu.make_async_copy(z_in, z_out, sem.at[1]),
    )
    for copy in copies:
        copy.start()
    for copy in copies:
        copy.wait()


def body(nz, nx, ny, right_side, inverse_diag, coupling, pattern):
    levels, rhs = right_side.shape[0], right_side.shape[4]
    pairs = levels - 1
    items = pairs * PANELS
    rows, cols = coupling.shape[2], coupling.shape[4]
    b = right_side.reshape(levels, W, rhs)
    d = inverse_diag.reshape(levels, W, W)
    m = coupling.reshape(pairs, rows, cols)
    gate = pattern.reshape(pairs, 2 * ny, nz * nx)
    hbm = pl.BlockSpec(memory_space=pltpu.HBM)
    vm = pl.BlockSpec(memory_space=pltpu.VMEM)
    b, d, gate = (pltpu.with_memory_space_constraint(x, pltpu.HBM) for x in (b, d, gate))
    f, z = pl.pallas_call(
        functools.partial(kernel, nz, nx, ny, levels),
        out_shape=[jax.ShapeDtypeStruct((levels, W, rhs), BF16)] * 2,
        in_specs=[hbm, hbm, hbm, hbm],
        out_specs=[vm, vm],
        scratch_shapes=[
            pltpu.VMEM((levels, W, rhs), BF16),
            pltpu.VMEM((levels, W, W), BF16),
            pltpu.VMEM((pairs, 2 * ny, nz * nx), jnp.int32),
            pltpu.VMEM((pairs, 2 * ny, 1, cols), F32),
            pltpu.VMEM((pairs, rows, cols), BF16),
            pltpu.VMEM((pairs, cols, rows), BF16),
            pltpu.VMEM((items, nz, nx, W, W), BF16),
            pltpu.VMEM((PANELS, W, W), F32),
            pltpu.VMEM((2 * ny, W, W), F32),
            pltpu.VMEM((PANELS, 2 * ny - 1, W, W), BF16),
            pltpu.VMEM((items, 2 * ny - 1, W, W), BF16),
            pltpu.VMEM((items, 2 * ny, W, W), BF16),
            pltpu.VMEM((PANELS, nz, nx, W, W), BF16),
            pltpu.VMEM((items, nz - 1, nx, H, W), BF16),
            pltpu.VMEM((items, nx - 1, nz, H, W), BF16),
            pltpu.VMEM((items, 2, nx - 1, H, W), BF16),
            pltpu.VMEM((items, 2, nx - 1, H, W), BF16),
            pltpu.VMEM((PANELS, W, W), F32),
            pltpu.VMEM((items + PANELS, W, W), BF16),
            pltpu.SemaphoreType.DMA((pairs,)),
            pltpu.SemaphoreType.DMA((2, levels)),
            pltpu.SemaphoreType.DMA,
            pltpu.SemaphoreType.DMA((6, items)),
            pltpu.SemaphoreType.DMA((6, items)),
        ],
        compiler_params=pltpu.CompilerParams(
            collective_id=0, has_side_effects=True, vmem_limit_bytes=50 * 1024 * 1024
        ),
    )(b, d, gate, m)
    shape = right_side.shape
    anywhere = pl.BlockSpec(memory_space=pl.ANY)
    f, z = pl.pallas_call(
        store,
        out_shape=[jax.ShapeDtypeStruct((levels, W, rhs), BF16)] * 2,
        in_specs=[anywhere, anywhere],
        out_specs=[anywhere, anywhere],
        scratch_shapes=[pltpu.SemaphoreType.DMA((2,))],
        compiler_params=pltpu.CompilerParams(vmem_limit_bytes=50 * 1024 * 1024),
    )(f, z)
    return f.reshape(shape), z.reshape(shape)


def solution(mesh):
    placed = (
        P(None, "row", ("depth", "col"), None, None),
        P(None, "row", ("depth", "col"), None, None, None),
        P(None, "row", None, ("depth", "col"), None),
        P(None, "row", None, ("depth", "col"), None),
    )
    side = round(mesh.shape["row"] ** 0.5)
    return jax.shard_map(
        functools.partial(body, side, side, mesh.shape["col"]),
        mesh=mesh,
        in_specs=placed,
        out_specs=(placed[0], placed[0]),
        check_vma=False,
    )
```

```python
import functools

import jax
import jax.numpy as jnp
from jax import lax
from jax.experimental import pallas as pl
from jax.experimental.pallas import tpu as pltpu
from jax.sharding import PartitionSpec as P

F32 = jnp.float32
BF16 = jnp.bfloat16
W = 128
H = 64
PANELS = 4


def far_first(n):
    return sorted(range(1, n), key=lambda k: -min(k, n - k))


def kernel(
    nz, nx, ny, levels,
    b_hbm, d_hbm, pat_hbm, m_hbm,
    fo, zo,
    bv, dv, pat, gate, mv, mt, xg, ownf, yf, ys, yr, yg, rs, rr0, rr1, ls, lr, ownb, ft,
    load_sem, in_sem, pat_sem, send_sem, recv_sem,
):
    pairs = levels - 1
    items = pairs * PANELS
    dd = lax.axis_index("depth")
    rw = lax.axis_index("row")
    yy = lax.axis_index("col")
    zz = rw // nx
    xx = rw % nx
    shares = [(flip, k) for k in far_first(ny) for flip in (0, 1)] + [(1, 0)]

    def x_peer(step):
        return {"row": zz * nx + (xx + step) % nx}

    def z_peer(step):
        return {"row": ((zz + step) % nz) * nx + xx}

    def share_peer(flip, step):
        return {"depth": (dd + flip) % 2, "col": (yy + step) % ny}

    peers = (
        [x_peer(k) for k in range(1, nx)]
        + [z_peer(k) for k in range(1, nz)]
        + [share_peer(*share) for share in shares]
    )

    barrier = pltpu.get_barrier_semaphore()
    for peer in peers:
        pl.semaphore_signal(
            barrier, inc=1, device_id=peer, device_id_type=pl.DeviceIdType.MESH
        )

    def load_coupling(lv):
        return pltpu.make_async_copy(m_hbm.at[lv], mv.at[lv], load_sem.at[lv])

    def load_inputs(lv):
        return (
            pltpu.make_async_copy(b_hbm.at[lv], bv.at[lv], in_sem.at[0, lv]),
            pltpu.make_async_copy(d_hbm.at[lv], dv.at[lv], in_sem.at[1, lv]),
        )

    load_pattern = pltpu.make_async_copy(pat_hbm, pat, pat_sem)
    for copy in load_inputs(0):
        copy.start()
    load_pattern.start()
    for copy in load_inputs(0):
        copy.wait()
    for lv in range(1, levels):
        for copy in load_inputs(lv):
            copy.start()
    for lv in range(pairs):
        load_coupling(lv).start()

    pl.semaphore_wait(barrier, len(peers))

    def send(src, dst, stage, item, peer):
        pltpu.make_async_remote_copy(
            src_ref=src,
            dst_ref=dst,
            send_sem=send_sem.at[stage, item],
            recv_sem=recv_sem.at[stage, item],
            device_id=peer,
            device_id_type=pl.DeviceIdType.MESH,
        ).start()

    def total(stage, item):
        return (
            xg.at[item, 0, 0 : nx - 1],
            xg.at[item, 0 : nz - 1],
            yr.at[item],
            yr.at[item],
            xg.at[item, 0 : nz - 1],
            xg.at[item, 0, 0 : nx - 1],
        )[stage]

    def arrived(stage, item):
        ref = total(stage, item)
        pltpu.make_async_copy(ref, ref, recv_sem.at[stage, item]).wait()

    def sent(stage, item):
        ref = total(stage, item)
        pltpu.make_async_copy(ref, ref, send_sem.at[stage, item]).wait()

    def columns(panel):
        return pl.ds(pl.multiple_of(panel * W, W), W)

    def f1(item):
        lv, pn = item // PANELS, item % PANELS
        prev = item - PANELS

        def finish(residual):
            value = lax.dot_general(
                residual, dv[lv], (((1,), (1,)), ((), ())), preferred_element_type=F32
            ).astype(BF16)

            @pl.when(lv < pairs)
            def _():
                xg[item, zz, xx] = value
                for k in far_first(nx):
                    here = xg.at[item, zz, xx, 0:H]
                    send(here, here, 0, item, x_peer(k))
                for k in far_first(nz):
                    here = xg.at[item, zz, xx, H:W]
                    send(here, here, 0, item, z_peer(k))

            ft[item] = value
            fo[lv, :, columns(pn)] = value.astype(F32).T.astype(BF16)

        given = bv[lv, :, columns(pn)].astype(F32).T

        @pl.when(lv == 0)
        def _():
            finish(given.astype(BF16))

        @pl.when(lv > 0)
        def _():
            arrived(2, prev)
            acc = ownf[pn]
            for k in range(2 * ny - 1):
                acc = acc + yr[prev, k].astype(F32)
            finish((given - acc).astype(BF16))

    def f2(item):
        arrived(0, item)
        for k in far_first(nz):
            here = xg.at[item, zz, :, 0:H]
            send(here, here, 1, item, z_peer(k))
        for k in far_first(nx):
            here = xg.at[item, :, xx, H:W]
            send(here, here, 1, item, x_peer(k))

    def f3(item):
        lv, pn = item // PANELS, item % PANELS

        @pl.when(item >= PANELS)
        def _():
            sent(2, item - PANELS)

        arrived(1, item)
        solved = jnp.concatenate(
            [xg[item, i, j] for i in range(nz) for j in range(nx)], axis=1
        )
        for side in (0, 1):
            span = slice(side * ny * W, (side + 1) * ny * W)
            part = jnp.dot(solved, mt[lv, :, span], preferred_element_type=F32)
            for j in range(ny):
                yf[side * ny + j] = part[:, j * W : (j + 1) * W]
            for k in far_first(ny):
                slot = (dd + side) % 2 * ny + k - 1
                ys[pn, slot] = yf[side * ny + (yy + k) % ny].astype(BF16)
                send(
                    ys.at[pn, slot], yr.at[item, slot], 2, item,
                    share_peer((dd + side) % 2, k),
                )
        ys[pn, ny - 1] = yf[(1 - dd) * ny + yy].astype(BF16)
        send(ys.at[pn, ny - 1], yr.at[item, ny - 1], 2, item, share_peer(1, 0))
        ownf[pn] = yf[dd * ny + yy]

    def b1(item):
        step, pn = item // PANELS, item % PANELS
        lv = levels - 1 - step
        prev = item - PANELS

        def finish(residual):
            value = jnp.dot(residual, dv[lv], preferred_element_type=F32).astype(BF16)

            @pl.when(step < pairs)
            def _():
                mine = dd * ny + yy
                yg[item, mine] = value
                here = yg.at[item, mine]
                for k in far_first(ny):
                    for side in (0, 1):
                        send(here, here, 3, item, share_peer((dd + side) % 2, k))
                send(here, here, 3, item, share_peer(1, 0))

            zo[lv, :, columns(pn)] = value.astype(F32).T.astype(BF16)

        @pl.when(step == 0)
        def _():
            finish(ft[lv * PANELS + pn])

        @pl.when(step > 0)
        def _():
            arrived(5, prev)
            acc0 = ownb[pn, 0:H]
            for k in range(nx - 1):
                acc0 = acc0 + lr[prev, 0, k].astype(F32)
            acc1 = ownb[pn, H:W]
            for k in range(nz - 1):
                acc1 = acc1 + lr[prev, 1, k].astype(F32)
            acc = jnp.concatenate([acc0, acc1], axis=0)
            finish((ft[lv * PANELS + pn].astype(F32) - acc).astype(BF16))

    def b3(item):
        lv, pn = pairs - 1 - item // PANELS, item % PANELS

        @pl.when(item >= PANELS)
        def _():
            sent(4, item - PANELS)

        arrived(3, item)
        solved = jnp.concatenate([yg[item, k] for k in range(2 * ny)], axis=1)
        for at in range(nz):
            span = slice(at * nx * W, (at + 1) * nx * W)
            part = jnp.dot(solved, mv[lv, :, span], preferred_element_type=F32).astype(BF16)
            for j in range(nx):
                rs[pn, at, j] = part[:, j * W : (j + 1) * W]
        for k in far_first(nz):
            at = (zz + k) % nz
            send(rs.at[pn, at, :, 0:H], rr0.at[item, k - 1], 4, item, z_peer(k))
        for k in far_first(nx):
            at = (xx + k) % nx
            send(rs.at[pn, :, at, H:W], rr1.at[item, k - 1], 4, item, x_peer(k))

    def b4(item):
        pn = item % PANELS
        arrived(4, item)
        for k in far_first(nx) + [0]:
            at = (xx + k) % nx
            acc = rs[pn, zz, at, 0:H].astype(F32)
            for j in range(nz - 1):
                acc = acc + rr0[item, j, at].astype(F32)
            if k == 0:
                ownb[pn, 0:H] = acc
            else:
                ls[item, 0, k - 1] = acc.astype(BF16)
                send(ls.at[item, 0, k - 1], lr.at[item, 0, k - 1], 5, item, x_peer(k))
        for k in far_first(nz) + [0]:
            at = (zz + k) % nz
            acc = rs[pn, at, xx, H:W].astype(F32)
            for j in range(nx - 1):
                acc = acc + rr1[item, j, at].astype(F32)
            if k == 0:
                ownb[pn, H:W] = acc
            else:
                ls[item, 1, k - 1] = acc.astype(BF16)
                send(ls.at[item, 1, k - 1], lr.at[item, 1, k - 1], 5, item, z_peer(k))

    def spread_pattern():
        cols = nz * nx * W
        spread = (
            lax.broadcasted_iota(jnp.int32, (nz * nx, cols), 1) // W
            == lax.broadcasted_iota(jnp.int32, (nz * nx, cols), 0)
        ).astype(BF16)
        for lv in range(pairs):
            rows = jnp.dot(
                pat[lv].astype(F32).astype(BF16), spread, preferred_element_type=F32
            )
            for t in range(2 * ny):
                gate[lv, t] = rows[t : t + 1, :]

    def mask(lv, quarter):
        for t in range(2 * ny // 4):
            row = quarter * (2 * ny // 4) + t
            span = pl.ds(pl.multiple_of(row * W, W), W)
            gated = mv[lv, span, :] * gate[lv, row].astype(BF16)
            mv[lv, span, :] = gated
            mt[lv, :, span] = gated.T

    def settle(item, stages):
        for st in stages:
            sent(st, item)

    def stage(fn, index, count, *extra):
        @pl.when((index >= 0) & (index < count))
        def _():
            fn(index, *extra)

    def first(item, carry):
        f1(item)
        return carry

    def second(item, carry):
        f2(item)
        return carry

    def slot(s, carry):
        j = s - items

        @pl.when(j <= items)
        def _():
            stage(b4, j - 3, items)

        @pl.when(s >= PANELS)
        def _():
            stage(f1, s, items + PANELS)

        stage(b1, j, items + PANELS)
        @pl.when(s > PANELS)
        def _():
            stage(f2, s - 1, items)


        ahead = s + PANELS - 2

        @pl.when((ahead >= PANELS) & (ahead < items))
        def _():
            @pl.when(ahead % PANELS == 0)
            def _():
                load_coupling(ahead // PANELS).wait()

            mask(ahead // PANELS, ahead % PANELS)

        @pl.when(s == 1)
        def _():
            lax.fori_loop(0, PANELS, second, 0)
            load_coupling(0).wait()
            for quarter in range(4):
                mask(0, quarter)

        stage(f3, s - 2, items)
        stage(b3, j - 1, items)

        @pl.when(j >= items)
        def _():
            stage(b4, j - 2, items)

        stage(settle, j - 1, items, (0, 1))
        stage(settle, j - 5, items, (3, 5))
        return carry

    lax.fori_loop(0, PANELS, first, 0)
    load_pattern.wait()
    spread_pattern()
    for lv in range(1, levels):
        for copy in load_inputs(lv):
            copy.wait()
    lax.fori_loop(1, 2 * items + PANELS, slot, 0)
    settle(items - 1, (3, 5))
    for item in range(items - PANELS, items):
        settle(item, (2, 4))

def store(f_in, z_in, f_out, z_out, sem):
    copies = (
        pltpu.make_async_copy(f_in, f_out, sem.at[0]),
        pltpu.make_async_copy(z_in, z_out, sem.at[1]),
    )
    for copy in copies:
        copy.start()
    for copy in copies:
        copy.wait()


def body(nz, nx, ny, right_side, inverse_diag, coupling, pattern):
    levels, rhs = right_side.shape[0], right_side.shape[4]
    pairs = levels - 1
    items = pairs * PANELS
    rows, cols = coupling.shape[2], coupling.shape[4]
    b = right_side.reshape(levels, W, rhs)
    d = inverse_diag.reshape(levels, W, W)
    m = coupling.reshape(pairs, rows, cols)
    gate = pattern.reshape(pairs, 2 * ny, nz * nx)
    hbm = pl.BlockSpec(memory_space=pltpu.HBM)
    vm = pl.BlockSpec(memory_space=pltpu.VMEM)
    b, d, gate = (pltpu.with_memory_space_constraint(x, pltpu.HBM) for x in (b, d, gate))
    f, z = pl.pallas_call(
        functools.partial(kernel, nz, nx, ny, levels),
        out_shape=[jax.ShapeDtypeStruct((levels, W, rhs), BF16)] * 2,
        in_specs=[hbm, hbm, hbm, hbm],
        out_specs=[vm, vm],
        scratch_shapes=[
            pltpu.VMEM((levels, W, rhs), BF16),
            pltpu.VMEM((levels, W, W), BF16),
            pltpu.VMEM((pairs, 2 * ny, nz * nx), jnp.int32),
            pltpu.VMEM((pairs, 2 * ny, 1, cols), F32),
            pltpu.VMEM((pairs, rows, cols), BF16),
            pltpu.VMEM((pairs, cols, rows), BF16),
            pltpu.VMEM((items, nz, nx, W, W), BF16),
            pltpu.VMEM((PANELS, W, W), F32),
            pltpu.VMEM((2 * ny, W, W), F32),
            pltpu.VMEM((PANELS, 2 * ny - 1, W, W), BF16),
            pltpu.VMEM((items, 2 * ny - 1, W, W), BF16),
            pltpu.VMEM((items, 2 * ny, W, W), BF16),
            pltpu.VMEM((PANELS, nz, nx, W, W), BF16),
            pltpu.VMEM((items, nz - 1, nx, H, W), BF16),
            pltpu.VMEM((items, nx - 1, nz, H, W), BF16),
            pltpu.VMEM((items, 2, nx - 1, H, W), BF16),
            pltpu.VMEM((items, 2, nx - 1, H, W), BF16),
            pltpu.VMEM((PANELS, W, W), F32),
            pltpu.VMEM((items + PANELS, W, W), BF16),
            pltpu.SemaphoreType.DMA((pairs,)),
            pltpu.SemaphoreType.DMA((2, levels)),
            pltpu.SemaphoreType.DMA,
            pltpu.SemaphoreType.DMA((6, items)),
            pltpu.SemaphoreType.DMA((6, items)),
        ],
        compiler_params=pltpu.CompilerParams(
            collective_id=0, has_side_effects=True, vmem_limit_bytes=50 * 1024 * 1024
        ),
    )(b, d, gate, m)
    shape = right_side.shape
    anywhere = pl.BlockSpec(memory_space=pl.ANY)
    f, z = pl.pallas_call(
        store,
        out_shape=[jax.ShapeDtypeStruct((levels, W, rhs), BF16)] * 2,
        in_specs=[anywhere, anywhere],
        out_specs=[anywhere, anywhere],
        scratch_shapes=[pltpu.SemaphoreType.DMA((2,))],
        compiler_params=pltpu.CompilerParams(vmem_limit_bytes=50 * 1024 * 1024),
    )(f, z)
    return f.reshape(shape), z.reshape(shape)


def solution(mesh):
    placed = (
        P(None, "row", ("depth", "col"), None, None),
        P(None, "row", ("depth", "col"), None, None, None),
        P(None, "row", None, ("depth", "col"), None),
        P(None, "row", None, ("depth", "col"), None),
    )
    side = round(mesh.shape["row"] ** 0.5)
    return jax.shard_map(
        functools.partial(body, side, side, mesh.shape["col"]),
        mesh=mesh,
        in_specs=placed,
        out_specs=(placed[0], placed[0]),
        check_vma=False,
    )
```
